32 devices in a mesh: section: 4 (over y, x), tensor: 8 (over z, core).
Axes of the slice: x: 2, y: 2, z: 4, core: 2. Of those that a mesh axis runs over, the one named last changes fastest.
Arguments:
- tokens: bfloat16 [2, 32, 4096], P(None, 'tensor'), may hold values from -24 to 24
- expert_ids: int32 [4, 2, 32, 2], P('section', None, 'tensor'), may hold values from 0 to 7, as said below
- router_weight: bfloat16 [4, 4096, 8], P('section'), may hold values from -0.09375 to 0.09375
- norm_gain: float32 [4, 4096], P('section'), may hold values from 0.1 to 1.9
- gate_weight: bfloat16 [4, 28672, 4096], P('section', 'tensor'), may hold values from -0.09375 to 0.09375
- up_weight: bfloat16 [4, 28672, 4096], P('section', 'tensor'), may hold values from -0.09375 to 0.09375
- down_weight: bfloat16 [4, 28672, 4096], P('section', 'tensor'), may hold values from -0.046875 to 0.046875
Outputs:
- section_outputs: bfloat16 [4, 2, 32, 4096], P('section', None, 'tensor')
The draws below stay inside these ranges and needn't reach their ends.
Inputs may be any that keep to these rules, and one draw needn't show every extreme that they name: `expert_ids`: each token names two different experts. Along the token dimension, in aligned blocks of 4 tokens of one micro-batch and one layer, at most 2 tokens name expert 0 and at most 2 name expert 1; in some micro-batch of every layer every block has exactly 2 of each.
All inputs are finite; a program needn't handle non-finite values.
Results may differ from the reference program's by a relative error of at most 0.0055.
Values may be sent and summed in bfloat16 or wider, within the bound.
A program may use at most 128 MiB of HBM per device.

```python
import math
import jax
import jax.numpy as jnp
from jax import lax

D = 4096
FF = 14336
EXPERTS = 8
MICRO = 2
TOK_DEV = 4
SLOT = 2
TOK = 32
N_SECTION = 4
N_TENSOR = 8


def draw_tokens(key, part):
    keys = jax.random.split(jax.random.fold_in(key, 11), 3)
    shape = (MICRO, TOK, D)
    row_scale = jnp.exp(jax.random.uniform(keys[0], (MICRO, TOK, 1), jnp.float32, math.log(0.5), math.log(2.0)))
    column_scale = jnp.exp(jax.random.uniform(keys[1], (1, 1, D), jnp.float32, math.log(0.4), math.log(4.0)))
    values = jax.random.normal(keys[2], shape, jnp.float32) * row_scale * column_scale
    return jnp.clip(values, -24.0, 24.0).astype(jnp.bfloat16)


def draw_expert_ids(key, part):
    keys = jax.random.split(jax.random.fold_in(key, 23), 8)
    shape = (N_SECTION, MICRO, N_TENSOR, TOK_DEV)
    full_micro = jax.random.randint(keys[0], (N_SECTION,), 0, MICRO)
    micro_index = jnp.arange(MICRO, dtype=jnp.int32)
    is_full = micro_index[None, :, None] == full_micro[:, None, None]
    counts_zero = jnp.where(is_full, SLOT, jax.random.randint(keys[1], (N_SECTION, MICRO, N_TENSOR), 0, SLOT + 1))
    counts_one = jnp.where(is_full, SLOT, jax.random.randint(keys[2], (N_SECTION, MICRO, N_TENSOR), 0, SLOT + 1))
    position = jnp.arange(TOK_DEV, dtype=jnp.int32)
    scores_zero = jax.random.randint(keys[3], shape, 0, 1 << 20) * TOK_DEV + position
    scores_one = jax.random.randint(keys[4], shape, 0, 1 << 20) * TOK_DEV + position
    rank_zero = jnp.argsort(jnp.argsort(scores_zero, axis=-1), axis=-1).astype(jnp.int32)
    rank_one = jnp.argsort(jnp.argsort(scores_one, axis=-1), axis=-1).astype(jnp.int32)
    names_zero = rank_zero < counts_zero[..., None]
    names_one = rank_one < counts_one[..., None]
    first_alt = 2 + jax.random.randint(keys[5], shape, 0, EXPERTS - 2)
    second_alt = 2 + (first_alt - 2 + 1 + jax.random.randint(keys[6], shape, 0, EXPERTS - 3)) % (EXPERTS - 2)
    first_id = jnp.where(names_zero, 0, jnp.where(names_one, 1, first_alt))
    second_id = jnp.where(names_zero, jnp.where(names_one, 1, first_alt), jnp.where(names_one, first_alt, second_alt))
    swapped = jax.random.randint(keys[7], shape, 0, 2) == 1
    routes = jnp.stack([jnp.where(swapped, second_id, first_id), jnp.where(swapped, first_id, second_id)], axis=-1)
    return routes.reshape(N_SECTION, MICRO, TOK, 2).astype(jnp.int32)


def block_scale(key, shape, cuts, least, high):
    def one(dim, shards_of):
        steps = jax.random.uniform(jax.random.fold_in(jax.random.fold_in(key, 6), dim), (shards_of,), jnp.float32, least / len(cuts), high / len(cuts))
        return jnp.repeat(jnp.exp(steps), shape[dim] // shards_of).reshape((-1,) + (1,) * (len(shape) - dim - 1))

    level = one(*cuts[0])
    for cut in cuts[1:]:
        level = level * one(*cut)
    return level


def normal_values(own_key, extent, spread, most, cuts=(), kind=jnp.bfloat16):
    entries = jax.random.normal(own_key, extent, jnp.float32) * spread
    if len(cuts) > 0:
        entries = block_scale(own_key, extent, cuts, -0.22, 0.18) * entries
    return jnp.clip(entries, min=-most, max=most).astype(kind)


def setup_inputs(seed: int = 0) -> dict:
    arg_keys = jax.random.split(jax.random.key(seed), 8)
    tokens = draw_tokens(jax.random.fold_in(arg_keys[7], 71), 0)
    expert_ids = draw_expert_ids(jax.random.fold_in(arg_keys[7], 71), 0)
    router_weight = normal_values(arg_keys[2], (N_SECTION, D, EXPERTS), D ** -0.5, 0.09375, ((0, 4),))
    norm_gain = jnp.clip(1.0 + 0.18 * jax.random.normal(arg_keys[3], (N_SECTION, D), jnp.float32), 0.1, 1.9)
    gate_weight = normal_values(arg_keys[4], (N_SECTION, 2 * FF, D), D ** -0.5, 0.09375, ((0, 4), (1, 8)))
    up_weight = normal_values(arg_keys[5], (N_SECTION, 2 * FF, D), D ** -0.5, 0.09375, ((0, 4), (1, 8)))
    down_weight = normal_values(arg_keys[6], (N_SECTION, 2 * FF, D), FF ** -0.5, 0.046875, ((0, 4), (1, 8)))
    return {"tokens": tokens, "expert_ids": expert_ids, "router_weight": router_weight, "norm_gain": norm_gain, "gate_weight": gate_weight, "up_weight": up_weight, "down_weight": down_weight}


EPSILON = 1e-05

def normalize(hidden_rows, gain):
    wide = hidden_rows.astype(jnp.float32)
    scale = lax.rsqrt(lax.optimization_barrier(jnp.mean(wide * wide, axis=-1, keepdims=True)) + EPSILON)
    return (wide * scale * gain).astype(jnp.bfloat16)

def mixing_weight(logits, routes, expert):
    routed = (routes[:, 0] == expert) | (routes[:, 1] == expert)
    partner = jnp.where(routes[:, 0] == expert, routes[:, 1], routes[:, 0])
    columns = jnp.arange(logits.shape[1], dtype=jnp.int32)
    partner_logit = lax.optimization_barrier(jnp.sum(jnp.where(columns[None, :] == partner[:, None], logits, 0.0), axis=1))
    value = 1.0 / (1.0 + jnp.exp(partner_logit - logits[:, expert]))
    return (jnp.where(routed, value, 0.0), routed.astype(jnp.int32))

def pickers(flags, slot_count):
    place = jnp.cumsum(flags, axis=1) - 1
    slots = jnp.arange(slot_count, dtype=jnp.int32)
    chosen = (place[:, None, :] == slots[None, :, None]) & (flags[:, None, :] == 1)
    return chosen.astype(jnp.float32)

def project_rows(rows, weight_rows):
    return lax.dot_general(rows, weight_rows, (((1,), (1,)), ((), ())), preferred_element_type=jnp.float32)

def one_layer(hidden_rows, routes, router, gain, w_gate, w_up, w_down):
    normed = normalize(hidden_rows, gain)
    logits = jnp.dot(normed, router, preferred_element_type=jnp.float32)
    blocks = normed.reshape(N_TENSOR, TOK_DEV, D).astype(jnp.float32)
    total = hidden_rows.astype(jnp.float32)
    for expert in range(2):
        weight, flags = mixing_weight(logits, routes, expert)
        picker = pickers(flags.reshape(N_TENSOR, TOK_DEV), SLOT)
        packed = jnp.einsum('bsj,bjd->bsd', picker, blocks, precision=lax.Precision.HIGHEST)
        packed = packed.astype(jnp.bfloat16).reshape(N_TENSOR * SLOT, D)
        gate = project_rows(packed, w_gate[expert * FF:(expert + 1) * FF])
        upward = project_rows(packed, w_up[expert * FF:(expert + 1) * FF])
        hidden = (jax.nn.silu(gate) * upward).astype(jnp.bfloat16)
        slot_out = jnp.dot(hidden, w_down[expert * FF:(expert + 1) * FF], preferred_element_type=jnp.float32)
        output = jnp.einsum('bsj,bsd->bjd', picker, slot_out.reshape(N_TENSOR, SLOT, D), precision=lax.Precision.HIGHEST)
        total = total + weight[:, None] * output.reshape(TOK, D)
    return total.astype(jnp.bfloat16)

def reference(tokens, expert_ids, router_weight, norm_gain, gate_weight, up_weight, down_weight):
    current = tokens
    collected = []
    for layer in range(N_SECTION):

        def run_micro(pair, layer=layer):
            return one_layer(pair[0], pair[1], router_weight[layer], norm_gain[layer], gate_weight[layer], up_weight[layer], down_weight[layer])
        current = lax.map(run_micro, (current, expert_ids[layer]))
        collected.append(current)
    return jnp.stack(collected)
```

```python
import functools

import jax
import jax.numpy as jnp
from jax import lax
from jax.experimental import pallas as pl
from jax.experimental.pallas import tpu as pltpu
from jax.sharding import PartitionSpec as P

EPSILON = 1e-05
PARTS = 4
MESH = pl.DeviceIdType.MESH


def kernel(
    n, sections, chunk, pairs, extra,
    ids, tokens, router, gain, w_gate, w_up, w_down, out,
    pool, h_in, h_out, mine, gathered, x, hidden, back, returned,
    gate_sem, down_sem, send_sem, recv_sem, back_sem, ret_sem, hop_send, hop_recv,
):
    section = lax.axis_index("section")
    me = lax.axis_index("tensor")
    half = n // 2
    group = me // half
    micro, count, width = tokens.shape
    slots = count // 2
    rows = micro * count
    packed = micro * slots
    part = width // PARTS
    total_slots = 2 * pairs + extra

    def weight_copy(source, j, which):
        place = 2 * j + which
        start = pl.multiple_of(j * chunk, chunk)
        return pltpu.make_async_copy(
            source.at[0, pl.ds(start, chunk), :], pool.at[place], gate_sem.at[place]
        )

    def down_place(block):
        return lax.rem(2 * pairs + block // PARTS, total_slots), block % PARTS

    def down_copy(block):
        place, column = down_place(block)
        row = pl.multiple_of((block % pairs) * chunk, chunk)
        source_column = pl.multiple_of((block // pairs) * part, part)
        column = pl.multiple_of(column * part, part)
        return pltpu.make_async_copy(
            w_down.at[0, pl.ds(row, chunk), pl.ds(source_column, part)],
            pool.at[place, :, pl.ds(column, part)],
            down_sem.at[block],
        )

    @pl.loop(0, pairs)
    def _(j):
        weight_copy(w_gate, j, 0).start()
        weight_copy(w_up, j, 1).start()

    for block in range(extra * PARTS):
        down_copy(block).start()

    barrier = pltpu.get_barrier_semaphore()

    @pl.loop(1, n)
    def _(k):
        pl.semaphore_signal(
            barrier, inc=1, device_id={"tensor": lax.rem(me + k, n)}, device_id_type=MESH
        )

    after = lax.rem(section + 1, sections)
    before = lax.rem(section + sections - 1, sections)
    for other in (after, before):
        pl.semaphore_signal(barrier, inc=1, device_id={"section": other}, device_id_type=MESH)
    pl.semaphore_wait(barrier, n + 1)

    row8 = lax.broadcasted_iota(jnp.int32, (rows, 128), 0)
    lane8 = lax.broadcasted_iota(jnp.int32, (rows, 128), 1)
    row_p = lax.broadcasted_iota(jnp.int32, (2 * packed, 128), 0)
    lane_p = lax.broadcasted_iota(jnp.int32, (2 * packed, 128), 1)
    pick = jnp.zeros((2 * packed, 128), jnp.float32)
    pick_t = jnp.zeros((rows, 128), jnp.float32)
    signs = []
    for expert in range(2):
        sign = jnp.zeros((rows, 128), jnp.float32)
        for m in range(micro):
            used = jnp.int32(0)
            for t in range(count):
                first = ids[0, m, t, 0]
                second = ids[0, m, t, 1]
                routed = (first == expert) | (second == expert)
                partner = jnp.where(first == expert, second, first)
                slot = expert * packed + m * slots + used
                slot = jnp.where(routed, slot, -1)
                used = used + routed.astype(jnp.int32)
                token = m * count + t
                pick = jnp.where((row_p == slot) & (lane_p == token), 1.0, pick)
                pick_t = jnp.where((row8 == token) & (lane8 == slot), 1.0, pick_t)
                sign = jnp.where((row8 == token) & (lane8 == partner), 1.0, sign)
        signs.append(sign - (lane8 == expert).astype(jnp.float32))

    hop = pltpu.make_async_remote_copy(
        src_ref=h_out, dst_ref=h_in, send_sem=hop_send, recv_sem=hop_recv,
        device_id={"section": after}, device_id_type=MESH,
    )

    @pl.when(section == 0)
    def _():
        h_in[...] = tokens[...]

    @pl.when(section > 0)
    def _():
        hop.wait_recv()

    h = jnp.concatenate([h_in[m].astype(jnp.float32) for m in range(micro)], axis=0)
    scale = lax.rsqrt(jnp.mean(h * h, axis=-1, keepdims=True) + EPSILON)
    normed = (h * scale * gain[...]).astype(jnp.bfloat16).astype(jnp.float32)
    chosen = pick[:, 0:1] * normed[0:1, :]
    for t in range(1, rows):
        chosen = chosen + pick[:, t : t + 1] * normed[t : t + 1, :]
    for expert in range(2):
        mine[expert] = chosen[expert * packed : (expert + 1) * packed].astype(jnp.bfloat16)

    def dispatch(peer):
        return pltpu.make_async_remote_copy(
            src_ref=mine.at[peer // half], dst_ref=gathered.at[me],
            send_sem=send_sem.at[peer], recv_sem=recv_sem.at[me],
            device_id={"tensor": peer}, device_id_type=MESH,
        )

    def arrival(peer):
        return pltpu.make_async_copy(mine.at[0], gathered.at[peer], recv_sem.at[peer])

    @pl.loop(1, n)
    def _(k):
        dispatch(lax.rem(me + k, n)).start()

    gathered[me] = mine[group]

    wide = jnp.concatenate([normed, normed], axis=0).astype(jnp.bfloat16)
    logits = jnp.dot(wide, router[0], preferred_element_type=jnp.float32)[:rows]
    experts = logits.shape[1]
    weights = []
    for expert in range(2):
        gap = jnp.sum(signs[expert][:, :experts] * logits, axis=1, keepdims=True)
        weights.append(1.0 / (1.0 + jnp.exp(gap)))
    coefficient = pick_t * jnp.where(lane8 < packed, weights[0], weights[1])

    @pl.loop(1, n)
    def _(k):
        arrival(lax.rem(me + k, n)).wait()

    step = 8 // packed
    for i in range(0, n, 2 * step):
        block = [gathered[i + a].astype(jnp.float32) for a in range(2 * step)]
        x[i * packed : (i + 2 * step) * packed, :] = jnp.concatenate(block, axis=0).astype(
            jnp.bfloat16
        )

    def project(place):
        return lax.dot_general(
            x[...], pool[place], (((1,), (1,)), ((), ())), preferred_element_type=jnp.float32
        )

    @pl.loop(0, pairs)
    def _(j):
        weight_copy(w_gate, j, 0).wait()
        gate = project(2 * j)
        weight_copy(w_up, j, 1).wait()
        upward = project(2 * j + 1)
        hidden[j] = (gate / (1.0 + jnp.exp(-gate)) * upward).astype(jnp.bfloat16)
        for a in range(2):
            late = 2 * j + extra + a

            @pl.when(late < pairs)
            def _():
                for b in range(PARTS):
                    down_copy(late * PARTS + b).start()

    def give_back(q, peer):
        return pltpu.make_async_remote_copy(
            src_ref=back.at[peer, q], dst_ref=returned.at[me, q],
            send_sem=back_sem.at[peer], recv_sem=ret_sem.at[me],
            device_id={"tensor": peer}, device_id_type=MESH,
        )

    for q in range(PARTS):
        for i in range(pairs):
            down_copy(q * pairs + i).wait()
        total = None
        for i in range(pairs):
            block = q * pairs + i
            place = (2 * pairs + block // PARTS) % total_slots
            column = (block % PARTS) * part
            term = jnp.dot(
                hidden[i], pool[place, :, column : column + part],
                preferred_element_type=jnp.float32,
            )
            total = term if total is None else total + term
        for i in range(n):
            back[i, q] = total[i * packed : (i + 1) * packed].astype(jnp.bfloat16)

        @pl.loop(1, n)
        def _(k):
            give_back(q, lax.rem(me + k, n)).start()

    returned[me] = back[me]

    @pl.loop(1, n)
    def _(k):
        peer = lax.rem(me + k, n)
        pltpu.make_async_copy(back.at[peer], returned.at[peer], ret_sem.at[peer]).wait()

    for q in range(PARTS):
        columns = slice(q * part, (q + 1) * part)
        sums = []
        for expert in range(2):
            value = returned[expert * half, q].astype(jnp.float32)
            for i in range(1, half):
                value = value + returned[expert * half + i, q].astype(jnp.float32)
            sums.append(value)
        result = jnp.concatenate([h_in[m, :, columns].astype(jnp.float32) for m in range(micro)], axis=0)
        for expert in range(2):
            for r in range(packed):
                slot = expert * packed + r
                result = result + coefficient[:, slot : slot + 1] * sums[expert][r : r + 1, :]
        for m in range(micro):
            h_out[m, :, columns] = result[m * count : (m + 1) * count].astype(jnp.bfloat16)

    @pl.when(section < sections - 1)
    def _():
        hop.start()

    out[0] = h_out[...]

    @pl.when(section < sections - 1)
    def _():
        hop.wait_send()

    @pl.loop(1, n)
    def _(k):
        peer = lax.rem(me + k, n)
        dispatch(peer).wait_send()
        pltpu.make_async_copy(back.at[peer], returned.at[peer], back_sem.at[peer]).wait()


def body(tokens, expert_ids, router_weight, norm_gain, gate_weight, up_weight, down_weight):
    n = lax.axis_size("tensor")
    sections = lax.axis_size("section")
    micro, count, width = tokens.shape
    packed = micro * count // 2
    held = gate_weight.shape[1]
    chunk = 256 if held % 256 == 0 else held
    pairs = held // chunk
    extra = min(2, pairs)
    bf16 = jnp.bfloat16
    vmem = pl.BlockSpec(memory_space=pltpu.VMEM)
    hbm = pl.BlockSpec(memory_space=pl.ANY)
    dma = pltpu.SemaphoreType.DMA
    return pl.pallas_call(
        functools.partial(kernel, n, sections, chunk, pairs, extra),
        out_shape=jax.ShapeDtypeStruct((1, micro, count, width), bf16),
        in_specs=[pl.BlockSpec(memory_space=pltpu.SMEM), vmem, vmem, vmem, hbm, hbm, hbm],
        out_specs=vmem,
        scratch_shapes=[
            pltpu.VMEM((2 * pairs + extra, chunk, width), bf16),
            pltpu.VMEM((micro, count, width), bf16),
            pltpu.VMEM((micro, count, width), bf16),
            pltpu.VMEM((2, packed, width), bf16),
            pltpu.VMEM((n, packed, width), bf16),
            pltpu.VMEM((n * packed, width), bf16),
            pltpu.VMEM((pairs, n * packed, chunk), bf16),
            pltpu.VMEM((n, PARTS, packed, width // PARTS), bf16),
            pltpu.VMEM((n, PARTS, packed, width // PARTS), bf16),
            dma((2 * pairs,)),
            dma((PARTS * pairs,)),
            dma((n,)),
            dma((n,)),
            dma((n,)),
            dma((n,)),
            dma,
            dma,
        ],
        compiler_params=pltpu.CompilerParams(
            collective_id=0, has_side_effects=True, vmem_limit_bytes=67043328
        ),
    )(expert_ids, tokens, router_weight, norm_gain, gate_weight, up_weight, down_weight)


def solution(mesh):
    return jax.shard_map(
        body,
        mesh=mesh,
        in_specs=(
            P(None, "tensor", None),
            P("section", None, "tensor", None),
            P("section", None, None),
            P("section", None),
            P("section", "tensor", None),
            P("section", "tensor", None),
            P("section", "tensor", None),
        ),
        out_specs=P("section", None, "tensor", None),
        check_vma=False,
    )
```
